512 devices in a mesh: lag: 16 (over y_lo, z), elem: 32 (over y_hi, x, core).
Axes of the slice: x: 4, y: 8 (y_hi: 4, y_lo: 2; y = y_hi * 2 + y_lo), z: 8, core: 2. Of those that a mesh axis runs over, the one named last changes fastest.
Arguments:
- kernel_tiles: bfloat16 [16, 32768, 1536], P('lag', 'elem'), may hold values from -0.0390625 to 0.0390625
- shell_index: int32 [16, 32, 3], P('lag', 'elem'), may hold values from 0 to 5
- cone_blocks: int32 [16], P('lag'), may hold values from 1 to 3
- history: bfloat16 [16, 32768, 256], P('lag', 'elem'), may hold values from -6 to 6
- prestress: float32 [32, 16, 64, 256], P('elem', 'lag'), may hold values from -6 to 6
- log_state: float32 [32, 16, 64, 256], P('elem', 'lag'), may hold values from -0.7 to 0.7
- fric_a: float32 [32, 16, 64], P('elem', 'lag'), may hold values from 0.3 to 1
- fric_b: float32 [32, 16, 64], P('elem', 'lag'), may hold values from 0.3 to 1
- normal_stress: float32 [32, 16, 64], P('elem', 'lag'), may hold values from 1 to 4
Outputs:
- final_rates: bfloat16 [32, 16, 64, 256], P('elem', 'lag')
- final_state: float32 [32, 16, 64, 256], P('elem', 'lag')
The draws below stay inside these ranges and needn't reach their ends.
Inputs may be any that keep to these rules, and one draw needn't show every extreme that they name: `shell_index`: 0 and 1 name the two blocks of the element block below the receiver block, 2 and 3 its own, 4 and 5 those of the block above.
All inputs are finite; a program needn't handle non-finite values.
Results may differ from the reference program's by a relative error of at most 0.0034.
Values may be sent and summed in bfloat16 or wider, within the bound.
A program may use at most 64 MiB of HBM per device.

```python
import math
import jax
import jax.numpy as jnp
from jax import lax

ELEM_DEV = 1024
BLOCK = 512
SHELL = 3
SCENARIOS = 256
STEPS = 4
NEWTON = 3
LAGS = 16
ELEMS = 32768
ROWS = 64
N_LAG = 16
N_ELEM = 32


def set_ends(entries, rng, smallest, high):
    longest = entries.shape.index(max(entries.shape))
    spots = []
    for shift in (0, 1):
        where = [jax.random.randint(jax.random.fold_in(rng, axis), (), 0, length) for axis, length in enumerate(entries.shape)]
        where[longest] = (where[longest] + shift) % entries.shape[longest]
        spots.append(tuple(where))
    return entries.at[spots[0]].set(smallest).at[spots[1]].set(high)


def steps_of(rng, extent, shards, least, top_value):
    gain, own = 1.0, jax.random.fold_in(rng, 6)
    for position, blocks in shards:
        heights = jnp.exp(jax.random.uniform(jax.random.fold_in(own, position), (blocks,), jnp.float32, least / len(shards), top_value / len(shards)))
        gain = gain * jnp.repeat(heights, extent[position] // blocks).reshape([-1 if axis == position else 1 for axis in range(len(extent))])
    return gain


def normal_values(own_key, extent, spread, most, pieces=(), kind=jnp.bfloat16):
    result = spread * jax.random.normal(own_key, extent, jnp.float32)
    if pieces:
        result = result * steps_of(own_key, extent, pieces, -0.22, 0.18)
    return jnp.clip(result, -most, most).astype(kind)


def setup_inputs(seed: int = 0) -> dict:
    seeds = jax.random.split(jax.random.key(seed), 10)
    return {
        "kernel_tiles": normal_values(seeds[0], (LAGS, ELEMS, SHELL * BLOCK), (SHELL * BLOCK * N_LAG) ** -0.5, 0.0390625, ((0, 16), (1, 32))),
        "shell_index": set_ends(jax.random.randint(seeds[1], (LAGS, N_ELEM, SHELL), 0, 6), jax.random.fold_in(seeds[1], 1), 0, 5).astype(jnp.int32),
        "cone_blocks": set_ends(jax.random.randint(seeds[2], (LAGS,), 1, SHELL + 1), jax.random.fold_in(seeds[2], 1), 1, SHELL).astype(jnp.int32),
        "history": normal_values(seeds[3], (LAGS, ELEMS, SCENARIOS), 1.0, 6.0, ((0, 16), (1, 32))),
        "prestress": normal_values(seeds[4], (N_ELEM, N_LAG, ROWS, SCENARIOS), 1.0, 6.0, ((0, 32), (1, 16)), jnp.float32),
        "log_state": jnp.clip(jax.random.uniform(seeds[5], (N_ELEM, N_LAG, ROWS, SCENARIOS), jnp.float32, -0.7, 0.7) * steps_of(seeds[5], (N_ELEM, N_LAG, ROWS, SCENARIOS), ((0, 32), (1, 16)), -0.4, 0.0), -0.7, 0.7),
        "fric_a": jnp.clip(jnp.exp(math.log(1.0) - 1.2039728 * jax.random.uniform(seeds[6], (N_ELEM, N_LAG, ROWS), jnp.float32) ** steps_of(seeds[6], (N_ELEM, N_LAG, ROWS), ((0, 32), (1, 16)), -0.2, 0.2)), 0.3, 1.0),
        "fric_b": jnp.clip(jnp.exp(math.log(1.0) - 1.2039728 * jax.random.uniform(seeds[7], (N_ELEM, N_LAG, ROWS), jnp.float32) ** steps_of(seeds[7], (N_ELEM, N_LAG, ROWS), ((0, 32), (1, 16)), -0.2, 0.2)), 0.3, 1.0),
        "normal_stress": jnp.clip(jnp.exp(math.log(4.0) - 1.3862944 * jax.random.uniform(seeds[8], (N_ELEM, N_LAG, ROWS), jnp.float32) ** steps_of(seeds[8], (N_ELEM, N_LAG, ROWS), ((0, 32), (1, 16)), -0.2, 0.2)), 1.0, 4.0),
    }


damping = 0.5
time_step = 0.25
creep_square = 0.01

def inverse_sinh(value):
    magnitude = jnp.abs(value)
    positive = jnp.log(magnitude + jnp.sqrt(magnitude * magnitude + 1.0))
    return jnp.where(value < 0.0, -positive, positive)

def gather_sources(lag_rates, shell_pick, live_count):
    padded = jnp.pad(lag_rates, ((ELEM_DEV, ELEM_DEV), (0, 0)))
    window_start = jnp.arange(N_ELEM, dtype=jnp.int32)[:, None] * ELEM_DEV + shell_pick.astype(jnp.int32) * BLOCK
    row_ids = window_start[:, :, None] + jnp.arange(BLOCK, dtype=jnp.int32)[None, None, :]
    sources = padded[row_ids]
    live_mask = jnp.arange(SHELL, dtype=jnp.int32)[None, :, None, None] < live_count
    sources = jnp.where(live_mask, sources, jnp.zeros((), sources.dtype))
    return sources.reshape(N_ELEM, SHELL * BLOCK, SCENARIOS)

def traction_sum(kernel_tiles, shell_index, cone_blocks, history):

    def one_lag(summed, items):
        kernel_tile, shell_pick, live_count, lag_rates = items
        sources = gather_sources(lag_rates, shell_pick, live_count)
        kernel_rows = kernel_tile.reshape(N_ELEM, ELEM_DEV, SHELL * BLOCK).astype(jnp.float32)
        partial_value = jnp.einsum('erc,ecs->ers', kernel_rows, sources.astype(jnp.float32))
        return (summed + partial_value.reshape(ELEMS, SCENARIOS), None)
    start_sum = jnp.zeros((ELEMS, SCENARIOS), jnp.float32)
    summed, unused = lax.scan(one_lag, start_sum, (kernel_tiles, shell_index, cone_blocks, history))
    return summed

def settle_friction(shear_load, state_now, coef_a, coef_b, sigma):
    scale = 0.5 * jnp.exp(coef_b / coef_a * state_now)
    strength = sigma * coef_a
    velocity = shear_load / (strength * scale + damping)
    for iteration in range(NEWTON):
        scaled = scale * velocity
        residual = strength * inverse_sinh(scaled) + damping * velocity - shear_load
        derivative = strength * scale / jnp.sqrt(1.0 + scaled * scaled) + damping
        velocity = velocity - residual / derivative
    speed = jnp.sqrt(velocity * velocity + creep_square)
    new_state = state_now + time_step * (jnp.exp(-state_now) - speed)
    return (velocity.astype(jnp.bfloat16), new_state)

def reference(kernel_tiles, shell_index, cone_blocks, history, prestress, log_state, fric_a, fric_b, normal_stress):
    stress_flat = prestress.reshape(ELEMS, SCENARIOS)
    state_flat = log_state.reshape(ELEMS, SCENARIOS)
    coef_a = fric_a.reshape(ELEMS, 1)
    coef_b = fric_b.reshape(ELEMS, 1)
    sigma = normal_stress.reshape(ELEMS, 1)
    lag_history = history
    slip_rate = history[0]
    for step_index in range(STEPS):
        traction = traction_sum(kernel_tiles, shell_index, cone_blocks, lag_history)
        slip_rate, state_flat = settle_friction(stress_flat + traction, state_flat, coef_a, coef_b, sigma)
        lag_history = jnp.concatenate([slip_rate[None], lag_history[:-1]], axis=0)
    final_rates = slip_rate.reshape(N_ELEM, N_LAG, ROWS, SCENARIOS)
    final_state = state_flat.reshape(N_ELEM, N_LAG, ROWS, SCENARIOS)
    return (final_rates, final_state)
```

```python
import functools

import jax
import jax.numpy as jnp
from jax import lax
from jax.experimental import pallas as pl
from jax.experimental.pallas import tpu as pltpu
from jax.sharding import PartitionSpec as P

SHELL = 3
STEPS = 4
NEWTON = 3
MESH = pl.DeviceIdType.MESH

damping = 0.5
time_step = 0.25
creep_square = 0.01


def inverse_sinh(value):
    magnitude = jnp.abs(value)
    positive = jnp.log(magnitude + jnp.sqrt(magnitude * magnitude + 1.0))
    return jnp.where(value < 0.0, -positive, positive)


def settle_friction(shear_load, state_now, coef_a, coef_b, sigma):
    scale = 0.5 * jnp.exp(coef_b / coef_a * state_now)
    strength = sigma * coef_a
    velocity = shear_load / (strength * scale + damping)
    for iteration in range(NEWTON):
        scaled = scale * velocity
        residual = strength * inverse_sinh(scaled) + damping * velocity - shear_load
        derivative = strength * scale / jnp.sqrt(1.0 + scaled * scaled) + damping
        velocity = velocity - residual / derivative
    speed = jnp.sqrt(velocity * velocity + creep_square)
    new_state = state_now + time_step * (jnp.exp(-state_now) - speed)
    return velocity.astype(jnp.bfloat16), new_state


def kernel(
    n_lag,
    n_elem,
    k_hbm,
    shell_ref,
    cone_ref,
    h_hbm,
    stress_hbm,
    state_hbm,
    a_ref,
    b_ref,
    s_ref,
    rates_ref,
    final_ref,
    kbuf,
    win,
    stage,
    recv,
    vst,
    stress,
    state,
    weights,
    src,
    load_sem,
    sem_b,
    sem_l,
    sem_r,
    sem_rs,
    send_x,
    send_s,
    send_rs,
    send_v,
):
    lag = lax.axis_index("lag")
    elem = lax.axis_index("elem")
    own, depth = kbuf.shape
    block = depth // SHELL
    blocks = 3 * own // block
    rows = own // n_lag
    odd = elem % 2
    partner = elem + 1 - 2 * odd
    other = elem - 1 + 2 * odd
    has_other = (other >= 0) & (other < n_elem)
    has_left = elem > 0
    has_right = elem < n_elem - 1
    is_root = lag == 0
    left_part, mid_part, right_part = (pl.ds(i * own, own) for i in range(3))

    def dev(l, e):
        return {"lag": l, "elem": e}

    load_k = pltpu.make_async_copy(k_hbm.at[0], kbuf, load_sem.at[0])
    load_h = pltpu.make_async_copy(h_hbm.at[0], win.at[0, mid_part], load_sem.at[1])
    load_p = pltpu.make_async_copy(stress_hbm.at[0, 0], stress, load_sem.at[2])
    load_s = pltpu.make_async_copy(state_hbm.at[0, 0], state, load_sem.at[3])
    load_h.start()
    load_k.start()
    load_p.start()
    load_s.start()

    barrier = pltpu.get_barrier_semaphore()

    def greet(i, carry):
        pl.semaphore_signal(
            barrier, inc=1, device_id=dev((lag + 1 + i) % n_lag, elem), device_id_type=MESH
        )
        return carry

    lax.fori_loop(0, n_lag - 1, greet, 0)

    @pl.when(has_left)
    def _():
        pl.semaphore_signal(barrier, inc=1, device_id=dev(lag, elem - 1), device_id_type=MESH)

    @pl.when(has_right)
    def _():
        pl.semaphore_signal(barrier, inc=1, device_id=dev(lag, elem + 1), device_id_type=MESH)

    @pl.when(is_root & has_other)
    def _():
        def greet_other(i, carry):
            pl.semaphore_signal(barrier, inc=1, device_id=dev(1 + i, other), device_id_type=MESH)
            return carry

        lax.fori_loop(0, n_lag - 1, greet_other, 0)

    @pl.when(jnp.logical_not(has_left))
    def _():
        for t in range(STEPS):
            win[t, left_part] = jnp.zeros((own, win.shape[2]), win.dtype)

    @pl.when(jnp.logical_not(has_right))
    def _():
        for t in range(STEPS):
            win[t, right_part] = jnp.zeros((own, win.shape[2]), win.dtype)

    greeters = n_lag - 1 + jnp.where(has_left, 1, 0) + jnp.where(has_right, 1, 0)
    greeters = greeters + jnp.where(jnp.logical_not(is_root) & has_other, 1, 0)
    pl.semaphore_wait(barrier, greeters)

    def put(src, dst, send_sem, recv_sem, where):
        pltpu.make_async_remote_copy(
            src_ref=src,
            dst_ref=dst,
            send_sem=send_sem,
            recv_sem=recv_sem,
            device_id=where,
            device_id_type=MESH,
        ).start()

    def wait_for(ref, sem):
        pltpu.make_async_copy(ref, ref, sem).wait()

    def exchange(t):
        @pl.when(has_left)
        def _():
            put(win.at[t, mid_part], win.at[t, right_part], send_x.at[t], sem_r.at[t], dev(lag, elem - 1))

        @pl.when(has_right)
        def _():
            put(win.at[t, mid_part], win.at[t, left_part], send_x.at[t], sem_l.at[t], dev(lag, elem + 1))

    def to_partner(t):
        @pl.when(odd == 1)
        def _():
            put(win.at[t, mid_part], win.at[t, right_part], send_x.at[t], sem_r.at[t], dev(lag, partner))

        @pl.when(odd == 0)
        def _():
            put(win.at[t, mid_part], win.at[t, left_part], send_x.at[t], sem_l.at[t], dev(lag, partner))

    def shift(t):
        @pl.when(lag < n_lag - 1)
        def _():
            put(win.at[t, mid_part], win.at[t + 1, mid_part], send_s.at[t], sem_b.at[t + 1], dev(lag + 1, elem))

    def wait_sides(t):
        @pl.when(has_left)
        def _():
            wait_for(win.at[t, left_part], sem_l.at[t])

        @pl.when(has_right)
        def _():
            wait_for(win.at[t, right_part], sem_r.at[t])

    tile = min(256, own)
    per_tile = tile // rows

    picks = shell_ref[0]
    live = cone_ref[...]
    for k in range(SHELL):
        for j in range(blocks):
            chosen = (picks[:, k : k + 1] == j) & (live > k)
            weight = jnp.broadcast_to(jnp.where(chosen, 1.0, 0.0), weights.shape[1:])
            weights[k * blocks + j] = weight.astype(weights.dtype)

    def pick_sources(t):
        strip = weights.shape[1]

        def one_strip(i, carry):
            pieces = [
                win[t, pl.ds(pl.multiple_of(j * block + i * strip, strip), strip), :]
                for j in range(blocks)
            ]
            for k in range(SHELL):
                value = pieces[0] * weights[k * blocks]
                for j in range(1, blocks):
                    value = value + pieces[j] * weights[k * blocks + j]
                src[pl.ds(pl.multiple_of(k * block + i * strip, strip), strip), :] = value
            return carry

        lax.fori_loop(0, block // strip, one_strip, 0)

    def products(t):
        pick_sources(t)

        def one_tile(j, carry):
            total = jnp.dot(
                kbuf[pl.ds(pl.multiple_of(j * tile, tile), tile), :],
                src[...],
                preferred_element_type=jnp.float32,
            )
            stage[t, pl.ds(pl.multiple_of(j * tile, tile), tile), :] = total.astype(stage.dtype)
            for q in range(per_tile):
                peer = j * per_tile + q

                @pl.when(peer != lag)
                def _():
                    put(
                        stage.at[t, pl.ds(pl.multiple_of(peer * rows, rows), rows)],
                        recv.at[t, (peer - lag - 1 + n_lag) % n_lag],
                        send_rs.at[t],
                        sem_rs.at[t],
                        dev(peer, elem),
                    )

            return carry

        lax.fori_loop(0, own // tile, one_tile, 0)

    def column(ref):
        row = lax.broadcasted_iota(jnp.int32, (rows, rows), 0)
        col = lax.broadcasted_iota(jnp.int32, (rows, rows), 1)
        return jnp.sum(jnp.where(row == col, ref[0], 0.0), axis=1, keepdims=True)

    def settle(t):
        wait_for(recv.at[t], sem_rs.at[t])
        total = stage[t, pl.ds(pl.multiple_of(lag * rows, rows), rows), :].astype(jnp.float32)
        for i in range(n_lag - 1):
            total = total + recv[t, i].astype(jnp.float32)
        rates, new_state = settle_friction(
            stress[...] + total, state[...], column(a_ref), column(b_ref), column(s_ref)
        )
        if t < STEPS - 1:
            state[...] = new_state
            vst[t] = rates
            spot = pl.ds(pl.multiple_of(lag * rows, rows), rows)

            @pl.when(jnp.logical_not(is_root))
            def _():
                put(
                    vst.at[t],
                    win.at[t + 1, pl.ds(pl.multiple_of(own + lag * rows, rows), rows)],
                    send_v.at[t],
                    sem_b.at[t + 1],
                    dev(0, elem),
                )

            @pl.when(is_root)
            def _():
                win[t + 1, pl.ds(own, rows)] = rates

            @pl.when(has_other & (odd == 1))
            def _():
                put(vst.at[t], win.at[t + 1, spot], send_v.at[t], sem_l.at[t + 1], dev(0, other))

            @pl.when(has_other & (odd == 0))
            def _():
                put(
                    vst.at[t],
                    win.at[t + 1, pl.ds(pl.multiple_of(2 * own + lag * rows, rows), rows)],
                    send_v.at[t],
                    sem_r.at[t + 1],
                    dev(0, other),
                )
        else:
            rates_ref[0, 0] = rates
            final_ref[0, 0] = new_state

    load_h.wait()
    exchange(0)
    shift(0)
    load_k.wait()
    load_p.wait()
    load_s.wait()
    wait_sides(0)
    products(0)
    for t in range(STEPS):
        if t + 1 < STEPS:

            @pl.when(jnp.logical_not(is_root))
            def _():
                wait_for(win.at[t + 1, mid_part], sem_b.at[t + 1])
                exchange(t + 1)

        settle(t)
        if t + 1 < STEPS:

            @pl.when(is_root)
            def _():
                wait_for(win.at[t + 1, pl.ds(own + rows, own - rows)], sem_b.at[t + 1])
                to_partner(t + 1)

            if t + 2 < STEPS:
                shift(t + 1)
            wait_sides(t + 1)
            products(t + 1)

    for t in range(STEPS):
        wait_for(recv.at[t], send_rs.at[t])
        if t == 0:

            @pl.when(has_left)
            def _():
                wait_for(win.at[t, mid_part], send_x.at[t])

            @pl.when(has_right)
            def _():
                wait_for(win.at[t, mid_part], send_x.at[t])

        else:

            @pl.when(is_root)
            def _():
                wait_for(win.at[t, mid_part], send_x.at[t])

            @pl.when(jnp.logical_not(is_root) & has_left)
            def _():
                wait_for(win.at[t, mid_part], send_x.at[t])

            @pl.when(jnp.logical_not(is_root) & has_right)
            def _():
                wait_for(win.at[t, mid_part], send_x.at[t])

        if t + 1 < STEPS:

            @pl.when(lag < n_lag - 1)
            def _():
                wait_for(win.at[t, mid_part], send_s.at[t])

            @pl.when(jnp.logical_not(is_root))
            def _():
                wait_for(vst.at[t], send_v.at[t])

            @pl.when(has_other)
            def _():
                wait_for(vst.at[t], send_v.at[t])


def shards(n_lag, n_elem, kernel_tiles, shell_index, cone_blocks, history, prestress, log_state, fric_a, fric_b, normal_stress):
    own, depth = kernel_tiles.shape[1:]
    rows, scenarios = prestress.shape[2:]
    half = jnp.bfloat16
    anywhere = pl.BlockSpec(memory_space=pl.ANY)
    local = pl.BlockSpec(memory_space=pltpu.VMEM)
    dma = pltpu.SemaphoreType.DMA
    return pl.pallas_call(
        functools.partial(kernel, n_lag, n_elem),
        out_shape=(
            jax.ShapeDtypeStruct((1, 1, rows, scenarios), half),
            jax.ShapeDtypeStruct((1, 1, rows, scenarios), jnp.float32),
        ),
        in_specs=[anywhere, local, local, anywhere, anywhere, anywhere, local, local, local],
        out_specs=(local, local),
        scratch_shapes=[
            pltpu.VMEM((own, depth), half),
            pltpu.VMEM((STEPS, 3 * own, scenarios), half),
            pltpu.VMEM((STEPS, own, scenarios), half),
            pltpu.VMEM((STEPS, n_lag - 1, rows, scenarios), half),
            pltpu.VMEM((STEPS, rows, scenarios), half),
            pltpu.VMEM((rows, scenarios), jnp.float32),
            pltpu.VMEM((rows, scenarios), jnp.float32),
            pltpu.VMEM((SHELL * 3 * own * SHELL // depth, 16, scenarios), half),
            pltpu.VMEM((depth, scenarios), half),
            dma((4,)),
            dma((STEPS,)),
            dma((STEPS,)),
            dma((STEPS,)),
            dma((STEPS,)),
            dma((STEPS,)),
            dma((STEPS,)),
            dma((STEPS,)),
            dma((STEPS,)),
        ],
        compiler_params=pltpu.CompilerParams(
            collective_id=0, has_side_effects=True, vmem_limit_bytes=48 * 1024 * 1024
        ),
    )(kernel_tiles, shell_index, cone_blocks.reshape(1, 1), history, prestress, log_state, fric_a, fric_b, normal_stress)


def solution(mesh):
    in_specs = (
        P("lag", "elem", None),
        P("lag", "elem", None),
        P("lag"),
        P("lag", "elem", None),
        P("elem", "lag", None, None),
        P("elem", "lag", None, None),
        P("elem", "lag", None),
        P("elem", "lag", None),
        P("elem", "lag", None),
    )
    out_specs = (P("elem", "lag", None, None), P("elem", "lag", None, None))
    body = functools.partial(shards, mesh.shape["lag"], mesh.shape["elem"])
    return jax.shard_map(body, mesh=mesh, in_specs=in_specs, out_specs=out_specs, check_vma=False)
```
